32 devices in a mesh: dp: 8 (over z, y), tensor: 4 (over x, core).
Axes of the slice: x: 2, y: 2, z: 4, core: 2. Of those that a mesh axis runs over, the one named last changes fastest.
Arguments:
- tokens: bfloat16 [16384, 4096], P('dp', 'tensor'), may hold values from -6 to 6
- cotangent: bfloat16 [16384, 1536], P('dp', 'tensor'), may hold values from -0.059814453 to 0.059814453
- seg_start: int32 [8, 2], P('dp'), may hold values from 0 to 1024, as said below
- seg_length: int32 [8, 2], P('dp'), may hold values from 0 to 1024, as said below
Outputs:
- weight_grad: float32 [4096, 2, 1536], P('dp', None, 'tensor')
The draws below stay inside these ranges and needn't reach their ends.
Inputs may be any that keep to these rules, and one draw needn't show every extreme that they name: Within each index of dp the 2 segments lie in expert order, packed from row 0 without gaps: seg_start is the running sum of seg_length before each expert. `seg_length`: each length is at most 1024; in every draw some expert on some index of dp has exactly 1024 rows. Rows after the last segment belong to no expert.
All inputs are finite; a program needn't handle non-finite values.
Results may differ from the reference program's by a relative error of at most 0.0003.
Values may be sent and summed in bfloat16 or wider, within the bound.
A program may use at most 128 MiB of HBM per device.

```python
import jax
import jax.numpy as jnp
from jax import lax

D = 4096
FF = 1536
E_W = 2
CAP = 1024
TOKENS = 16384
N_DP = 8


def segment_bounds(key):
    keys = jax.random.split(jax.random.fold_in(key, 7), 4)
    load = jax.random.randint(keys[0], (N_DP, 1), 1, 5)
    lower = load * CAP // 8
    upper = load * CAP // 4 + 1
    draws = jax.random.randint(keys[1], (N_DP, E_W), 0, 1 << 30)
    length = lower + draws % (upper - lower)
    busy_device = jax.random.randint(keys[2], (), 0, N_DP)
    busy_expert = jax.random.randint(keys[3], (), 0, E_W)
    hit = (jnp.arange(N_DP)[:, None] == busy_device) & (jnp.arange(E_W)[None, :] == busy_expert)
    length = jnp.where(hit, CAP, length)
    start = jnp.cumsum(length, axis=1) - length
    return (start.astype(jnp.int32), length.astype(jnp.int32))


def draw_seg_start(key, part):
    return segment_bounds(key)[0]


def draw_seg_length(key, part):
    return segment_bounds(key)[1]


def with_spikes(values, rng, source, target, shards_of, factor):
    owner, partner = [(jnp.arange(values.shape[axis_at]) // (values.shape[axis_at] // shards_of)).reshape([-1 if axis == axis_at else 1 for axis in range(values.ndim)]) for axis_at in (source, target)]
    chosen = jax.random.permutation(rng, shards_of)[partner]
    strong = (owner == chosen) | (owner == (partner + shards_of // 2) % shards_of)
    return jnp.where(strong, factor * values, values)


def level_of(own_key, extent, shards, low, high):
    factor_of = 1.0
    for position, parts in shards:
        steps = jax.random.uniform(jax.random.fold_in(jax.random.fold_in(own_key, 6), position), (parts,), jnp.float32, low / len(shards), high / len(shards))
        factor_of = factor_of * jnp.repeat(jnp.exp(steps), extent[position] // parts).reshape((-1,) + (1,) * (len(extent) - 1 - position))
    return factor_of


def noise(key, extent, scale, bound, cuts=(), kind=jnp.bfloat16):
    values = jax.random.normal(key, extent, jnp.float32) * scale
    if len(cuts) > 0:
        values = level_of(key, extent, cuts, -0.22, 0.18) * values
    return jnp.clip(values, min=-bound, max=bound).astype(kind)


def bell_draw_with(stream_key, shape, width, bound, cuts, heavy, kind=jnp.bfloat16):
    drawn = width * jax.random.normal(stream_key, shape, jnp.float32)
    if cuts:
        drawn = drawn * level_of(stream_key, shape, cuts, -0.22, 0.18)
    return jnp.clip(with_spikes(drawn, jax.random.fold_in(stream_key, 3), *heavy), -bound, bound).astype(kind)


def setup_inputs(seed: int = 0) -> dict:
    splits = jax.random.split(jax.random.key(seed), 5)
    tokens = bell_draw_with(splits[0], (TOKENS, D), 1.0, 6.0, ((0, 8), (1, 4)), (0, 1, 8, 2.0))
    cotangent = noise(splits[1], (TOKENS, FF), 0.01, 0.059814453, ((0, 8), (1, 4)))
    seg_start = draw_seg_start(jax.random.fold_in(splits[4], 71), 0)
    seg_length = draw_seg_length(jax.random.fold_in(splits[4], 71), 0)
    return dict(tokens=tokens, cotangent=cotangent, seg_start=seg_start, seg_length=seg_length)


def reference(tokens, cotangent, seg_start, seg_length):
    tok = E_W * CAP

    def peer(total, index):
        rows_x = lax.dynamic_slice_in_dim(tokens, index * tok, tok, 0)
        rows_g = lax.dynamic_slice_in_dim(cotangent, index * tok, tok, 0)
        terms = []
        for expert in range(E_W):
            start = seg_start[index, expert].astype(jnp.int32)
            length = seg_length[index, expert].astype(jnp.int32)
            first = jnp.minimum(start, tok - CAP).astype(jnp.int32)
            rows = first + jnp.arange(CAP, dtype=jnp.int32)
            keep = (rows >= start) & (rows < start + length)
            block_x = lax.dynamic_slice_in_dim(rows_x, first, CAP, 0)
            block_g = lax.dynamic_slice_in_dim(rows_g, first, CAP, 0)
            block_g = jnp.where(keep[:, None], block_g, jnp.zeros_like(block_g))
            terms.append(jnp.dot(block_x.T, block_g, preferred_element_type=jnp.float32))
        return total + jnp.stack(terms, 1), None

    start_total = jnp.zeros((D, E_W, FF), jnp.float32)
    total, unused = lax.scan(peer, start_total, jnp.arange(N_DP, dtype=jnp.int32))
    return total
```

```python
import functools

import jax
import jax.numpy as jnp
from jax import lax
from jax.experimental import pallas as pl
from jax.experimental.pallas import tpu as pltpu
from jax.sharding import PartitionSpec as P

CAP = 1024
SUB = 128
STEPS = 32767.0
TINY = 1e-30
MESH = pl.DeviceIdType.MESH


def block_term(columns, grads, lower, upper, size):
    total_rows = columns.shape[0]
    first = jnp.minimum(lower, total_rows - size)
    rows = first + jnp.arange(size, dtype=jnp.int32)
    keep = (rows >= lower) & (rows < upper)
    block_x = lax.dynamic_slice_in_dim(columns, first, size, 0)
    block_g = lax.dynamic_slice_in_dim(grads, first, size, 0)
    block_g = jnp.where(keep[:, None], block_g, jnp.zeros_like(block_g))
    return lax.dot_general(
        block_x, block_g, (((0,), (0,)), ((), ())), preferred_element_type=jnp.float32
    )


def plain_device(tokens, cotangent, seg_start, seg_length):
    whole = lax.all_gather(tokens, "tensor", axis=1, tiled=True)
    terms = []
    for expert in range(seg_start.shape[1]):
        start = seg_start[0, expert]
        upper = start + seg_length[0, expert]
        terms.append(block_term(whole, cotangent, start, upper, CAP))
    return lax.psum_scatter(jnp.stack(terms, 1), "dp", scatter_dimension=0, tiled=True)


def unit_order(n_ff):
    if n_ff == 3:
        return [
            (0, 0), (1, 0), (0, 1), (2, 0), (3, 0), (1, 1),
            (2, 1), (3, 1), (1, 2), (2, 2), (3, 2), (0, 2),
        ]
    return [(r, f) for f in range(n_ff) for r in range(4)]


def line_order(units):
    if len(units) == 12:
        return [0, 1, 2, 5, 3, 4, 6, 8, 7, 9, 10, 11]
    return list(range(len(units)))


def pick(values, i):
    found = jnp.int32(values[0])
    for k in range(1, len(values)):
        found = jnp.where(i == k, values[k], found)
    return found


def scaled(value):
    top = jnp.maximum(jnp.max(jnp.abs(value), axis=0, keepdims=True), TINY)
    return jnp.round(value * (STEPS / top)).astype(jnp.int32), top * (1.0 / STEPS)


def grad_kernel(
    n_dp, n_t, experts, tok_ref, cot_ref, start_ref, length_ref, out_ref,
    xv, xt, gbuf, gm, acc, work,
    y_out, y_in, c_out, c_in, z_out, z_in,
    y_out_s, y_in_s, c_out_s, c_in_s, z_out_s, z_in_s,
    load_sem, g_send, g_recv, y_send, y_recv, c_send, c_recv, z_send, z_recv,
):
    d = lax.axis_index("dp")
    t = lax.axis_index("tensor")
    line = n_dp // 2
    z, y = d // 2, d % 2
    x, c = t // 2, t % 2
    rows = cot_ref.shape[0]
    n_ff = gbuf.shape[1]
    half = xv.shape[2]
    tall = half // 2
    units = unit_order(n_ff)
    count = 2 * len(units)
    on_line = line_order(units)
    unit_r = [r for r, f in units]
    unit_f = [f for r, f in units]

    def rel(r):
        return 2 * ((x + r // 2) % 2) + (c + r % 2) % 2

    pair = (d + 1 - 2 * y, t)
    partner, across = (d, rel(1)), (d, rel(2))

    loads = []
    for f in range(n_ff):
        loads.append(pltpu.make_async_copy(
            cot_ref.at[:, pl.ds(f * SUB, SUB)], gbuf.at[0, f], load_sem.at[f]))
    for p, parity in enumerate((1 - y, y)):
        at = pl.ds(pl.multiple_of(parity * half, half), half)
        loads.append(pltpu.make_async_copy(tok_ref.at[:, at], xv.at[p], load_sem.at[n_ff + p]))
    for f in [n_ff, 0] + list(range(1, n_ff)) + [n_ff + 1]:
        loads[f].start()

    barrier = pltpu.get_barrier_semaphore()
    for device in [pair] + [(d, rel(r)) for r in range(1, 4)]:
        pl.semaphore_signal(barrier, inc=1, device_id=device, device_id_type=MESH)

    @pl.when(z > 0)
    def _():
        pl.semaphore_signal(barrier, inc=1, device_id=(d - 2, t), device_id_type=MESH)

    @pl.when(z < line - 1)
    def _():
        pl.semaphore_signal(barrier, inc=1, device_id=(d + 2, t), device_id_type=MESH)

    ends = jnp.where(z > 0, 1, 0) + jnp.where(z < line - 1, 1, 0)
    pl.semaphore_wait(barrier, 4 + ends)

    def remote(src, dst, send, recv, device):
        return pltpu.make_async_remote_copy(
            src_ref=src, dst_ref=dst, send_sem=send, recv_sem=recv,
            device_id=device, device_id_type=MESH,
        )

    def g_copy(r, f):
        if r == 3:
            return remote(gbuf.at[2, f], gbuf.at[3, f], g_send.at[3, f], g_recv.at[3, f], partner)
        src = cot_ref.at[:, pl.ds(f * SUB, SUB)]
        return remote(
            src, gbuf.at[r, f], g_send.at[r, f], g_recv.at[r, f], partner if r == 1 else across)

    for f in range(n_ff):
        g_copy(2, f).start()
        g_copy(1, f).start()

    def y_copies(s):
        return (
            remote(y_out.at[s], y_in.at[s], y_send.at[0, s], y_recv.at[0, s], pair),
            remote(y_out_s.at[s], y_in_s.at[s], y_send.at[1, s], y_recv.at[1, s], pair),
        )

    def c_copies(s, r):
        device = (d, rel(r))
        return (
            remote(c_out.at[s], c_in.at[s], c_send.at[0, s], c_recv.at[0, s], device),
            remote(c_out_s.at[s], c_in_s.at[s], c_send.at[1, s], c_recv.at[1, s], device),
        )

    def z_copies(s, way):
        device = (d + 2 - 4 * way, t)
        return (
            remote(z_out.at[s], z_in.at[way, s], z_send.at[0, s], z_recv.at[way, 0, s], device),
            remote(z_out_s.at[s], z_in_s.at[way, s], z_send.at[1, s], z_recv.at[way, 1, s], device),
        )

    def unscaled(data, scale):
        return data[...].astype(jnp.int32).astype(jnp.float32) * scale[...]

    def put(value, data, scale):
        whole, step = scaled(value)
        data[...] = whole.astype(jnp.int16)
        scale[...] = step

    chunk = 256

    def turn(p):
        @pl.loop(0, rows // chunk)
        def _(i):
            at = pl.ds(pl.multiple_of(i * chunk, chunk), chunk)
            for b in range(half // SUB):
                block = xv[p, at, b * SUB : (b + 1) * SUB].astype(jnp.float32).T
                h, low = b * SUB // tall, b * SUB % tall
                xt[p, h, low : low + SUB, at] = block.astype(xt.dtype)

    loads[n_ff].wait()
    turn(0)

    def form(s):
        u, h = s // 2, s % 2
        r, f = pick(unit_r, u), pick(unit_f, u)

        @pl.when(h == 0)
        def _():
            for k in range(n_ff):
                @pl.when((r == 0) & (f == k))
                def _():
                    loads[k].wait()

                @pl.when((r == 1) & (f == k))
                def _():
                    g_copy(1, k).wait_recv()

                @pl.when((r == 2) & (f == k))
                def _():
                    g_copy(2, k).wait_recv()
                    g_copy(3, k).start()

                @pl.when((r == 3) & (f == k))
                def _():
                    g_copy(3, k).wait_recv()

            @pl.loop(0, rows // chunk)
            def _(i):
                at = pl.ds(pl.multiple_of(i * chunk, chunk), chunk)
                block = gbuf[r, f, at, :].astype(jnp.float32)
                row = i * chunk + lax.broadcasted_iota(jnp.int32, (chunk, SUB), 0)
                for e in range(experts):
                    low = start_ref[0, e]
                    keep = (row >= low) & (row < low + length_ref[0, e])
                    gm[at, e * SUB : (e + 1) * SUB] = jnp.where(keep, block, 0.0).astype(gm.dtype)

        value = jnp.dot(xt[0, h], gm[...], preferred_element_type=jnp.float32)
        put(value, y_out.at[s], y_out_s.at[s])
        for copy in y_copies(s):
            copy.start()

        @pl.when(s == 0)
        def _():
            loads[n_ff + 1].wait()
            turn(1)

        acc[s] = jnp.dot(xt[1, h], gm[...], preferred_element_type=jnp.float32)

    def join(s):
        r = pick(unit_r, s // 2)
        for copy in y_copies(s):
            copy.wait_recv()
        value = acc[s] + unscaled(y_in.at[s], y_in_s.at[s])

        @pl.when(r == 0)
        def _():
            put(value, c_in.at[s], c_in_s.at[s])

        @pl.when(r != 0)
        def _():
            put(value, c_out.at[s], c_out_s.at[s])
            for copy in c_copies(s, r):
                copy.start()

    def at_line(j):
        u = pick(on_line, j // 2)
        r = pick(unit_r, u)
        return 2 * u + j % 2, r, rel(r), pick(unit_f, u)

    def gather(s, r, ways):
        @pl.when(r != 0)
        def _():
            for copy in c_copies(s, r):
                copy.wait_recv()

        work[...] = unscaled(c_in.at[s], c_in_s.at[s])
        for way in ways:
            @pl.when(z > 0 if way == 0 else z < line - 1)
            def _():
                for copy in z_copies(s, way):
                    copy.wait_recv()
                work[...] += unscaled(z_in.at[way, s], z_in_s.at[way, s])

    def pass_on(j, way):
        s, r, to, f = at_line(j)
        further = to > z if way == 0 else to < z

        @pl.when((j >= 0) & (j < count) & further)
        def _():
            gather(s, r, (way,))
            put(work[...], z_out.at[s], z_out_s.at[s])
            for copy in z_copies(s, way):
                copy.start()

    def finish(j):
        s, r, to, f = at_line(j)

        @pl.when((j >= 0) & (j < count) & (to == z))
        def _():
            gather(s, r, (0, 1))
            down = pl.ds(pl.multiple_of((j % 2) * tall, tall), tall)
            along = pl.ds(pl.multiple_of(f * SUB, SUB), SUB)
            for e in range(experts):
                out_ref[e, down, along] = work[:, e * SUB : (e + 1) * SUB]

    JOIN, LINE, HOP = 4, 9, 2

    @pl.loop(0, count + LINE + HOP * (line - 1))
    def _(i):
        @pl.when(i < count)
        def _():
            form(i)

        @pl.when((i >= JOIN) & (i < count + JOIN))
        def _():
            join(i - JOIN)

        pass_on(i - LINE - HOP * z, 0)
        pass_on(i - LINE - HOP * (line - 1 - z), 1)
        finish(i - LINE - HOP * jnp.maximum(z, line - 1 - z))

    @pl.loop(0, count)
    def _(s):
        r = pick(unit_r, s // 2)
        to = rel(r)
        for copy in y_copies(s):
            copy.wait_send()

        @pl.when(r != 0)
        def _():
            for copy in c_copies(s, r):
                copy.wait_send()

        for way in range(2):
            @pl.when(to > z if way == 0 else to < z)
            def _():
                for copy in z_copies(s, way):
                    copy.wait_send()

    for f in range(n_ff):
        for r in range(1, 4):
            g_copy(r, f).wait_send()


def kernel_device(n_dp, n_t, tokens, cotangent, seg_start, seg_length):
    rows, width = tokens.shape
    ff = cotangent.shape[1]
    experts = seg_start.shape[1]
    half = width // 2
    tall = half // 2
    n_ff = ff // SUB
    count = 2 * n_t * n_ff
    wide = experts * SUB
    dma = pltpu.SemaphoreType.DMA
    anywhere = pl.BlockSpec(memory_space=pl.ANY)
    scalars = pl.BlockSpec(memory_space=pltpu.SMEM)
    data = pltpu.VMEM((count, tall, wide), jnp.int16)
    scale = pltpu.VMEM((count, 1, wide), jnp.float32)
    out = pl.pallas_call(
        functools.partial(grad_kernel, n_dp, n_t, experts),
        out_shape=jax.ShapeDtypeStruct((experts, half, ff), jnp.float32),
        in_specs=[anywhere, anywhere, scalars, scalars],
        out_specs=pl.BlockSpec(memory_space=pltpu.VMEM),
        scratch_shapes=[
            pltpu.VMEM((2, rows, half), tokens.dtype),
            pltpu.VMEM((2, 2, tall, rows), tokens.dtype),
            pltpu.VMEM((n_t, n_ff, rows, SUB), cotangent.dtype),
            pltpu.VMEM((rows, wide), cotangent.dtype),
            pltpu.VMEM((count, tall, wide), jnp.float32),
            pltpu.VMEM((tall, wide), jnp.float32),
            data, data, data, data, data,
            pltpu.VMEM((2, count, tall, wide), jnp.int16),
            scale, scale, scale, scale, scale,
            pltpu.VMEM((2, count, 1, wide), jnp.float32),
            dma((n_ff + 2,)),
            dma((n_t, n_ff)),
            dma((n_t, n_ff)),
            dma((2, count)),
            dma((2, count)),
            dma((2, count)),
            dma((2, count)),
            dma((2, count)),
            dma((2, 2, count)),
        ],
        compiler_params=pltpu.CompilerParams(
            collective_id=0, has_side_effects=True, vmem_limit_bytes=67043328
        ),
    )(tokens, cotangent, seg_start, seg_length)
    return out.transpose(1, 0, 2)


def solution(mesh):
    n_dp, n_t = mesh.shape["dp"], mesh.shape["tensor"]
    body = plain_device
    if n_t == 4 and n_dp == 2 * n_t:
        body = functools.partial(kernel_device, n_dp, n_t)
    in_specs = (P("dp", "tensor"), P("dp", "tensor"), P("dp", None), P("dp", None))
    out_specs = P("dp", None, "tensor")
    return jax.shard_map(
        body, mesh=mesh, in_specs=in_specs, out_specs=out_specs, check_vma=False
    )
```

```python
import functools

import jax
import jax.numpy as jnp
from jax import lax
from jax.experimental import pallas as pl
from jax.experimental.pallas import tpu as pltpu
from jax.sharding import PartitionSpec as P

CAP = 1024
SUB = 128
STEPS = 32767.0
TINY = 1e-30
JOIN, MERGE, LAST = 4, 2, 5
MESH = pl.DeviceIdType.MESH


def block_term(columns, grads, lower, upper, size):
    total_rows = columns.shape[0]
    first = jnp.minimum(lower, total_rows - size)
    rows = first + jnp.arange(size, dtype=jnp.int32)
    keep = (rows >= lower) & (rows < upper)
    block_x = lax.dynamic_slice_in_dim(columns, first, size, 0)
    block_g = lax.dynamic_slice_in_dim(grads, first, size, 0)
    block_g = jnp.where(keep[:, None], block_g, jnp.zeros_like(block_g))
    return lax.dot_general(
        block_x, block_g, (((0,), (0,)), ((), ())), preferred_element_type=jnp.float32
    )


def plain_device(tokens, cotangent, seg_start, seg_length):
    whole = lax.all_gather(tokens, "tensor", axis=1, tiled=True)
    terms = []
    for expert in range(seg_start.shape[1]):
        start = seg_start[0, expert]
        upper = start + seg_length[0, expert]
        terms.append(block_term(whole, cotangent, start, upper, CAP))
    return lax.psum_scatter(jnp.stack(terms, 1), "dp", scatter_dimension=0, tiled=True)


def unit_order(n_ff):
    if n_ff == 3:
        return [
            (0, 0), (1, 0), (1, 1), (1, 2), (2, 0), (3, 0),
            (2, 1), (3, 1), (2, 2), (3, 2), (0, 1), (0, 2),
        ]
    return [(r, f) for f in range(n_ff) for r in range(4)]


def pick(values, i):
    found = jnp.int32(values[0])
    for k in range(1, len(values)):
        found = jnp.where(i == k, values[k], found)
    return found


def grad_kernel(
    n_dp, n_t, experts, tok_ref, cot_ref, start_ref, length_ref, out_ref,
    xv, xt, gbuf, gm, acc, fresh, result, y_out, y_in, w_out, w_in,
    y_out_s, y_in_s, w_out_s, w_in_s,
    load_sem, g_send, g_recv, y_send, y_recv, w_send, w_recv, f_send, f_recv, store_sem,
):
    d = lax.axis_index("dp")
    t = lax.axis_index("tensor")
    line = n_dp // 2
    z, y = d // 2, d % 2
    x, c = t // 2, t % 2
    rows = cot_ref.shape[0]
    n_ff = gbuf.shape[1]
    tall = xv.shape[3]
    half = 2 * tall
    units = unit_order(n_ff)
    count = 2 * len(units)
    unit_r = [r for r, f in units]
    unit_f = [f for r, f in units]

    def unit_of(s):
        return 2 * (s // 4) + s % 2

    def rel(r):
        return 2 * ((x + r // 2) % 2) + (c + r % 2) % 2

    pair = (d + 1 - 2 * y, t)
    partner, across = (d, rel(1)), (d, rel(2))

    loads = {}
    for f in range(n_ff):
        loads[f] = pltpu.make_async_copy(
            cot_ref.at[:, pl.ds(f * SUB, SUB)], gbuf.at[0, f], load_sem.at[f])
    for p, parity in enumerate((1 - y, y)):
        for h in range(2):
            at = pl.ds(pl.multiple_of(parity * half + h * tall, tall), tall)
            loads[p, h] = pltpu.make_async_copy(
                tok_ref.at[:, at], xv.at[p, h], load_sem.at[n_ff + 2 * p + h])
    for name in [(0, 0), 0, (1, 0), (0, 1), (1, 1)] + list(range(1, n_ff)):
        loads[name].start()

    barrier = pltpu.get_barrier_semaphore()
    others = [(2 * ((z + k) % line) + y, t) for k in range(1, line)]
    for device in [pair] + [(d, rel(r)) for r in range(1, 4)] + others:
        pl.semaphore_signal(barrier, inc=1, device_id=device, device_id_type=MESH)
    pl.semaphore_wait(barrier, 4 + len(others))

    target = z == t
    merger = ((z == 1) & (t >= 2)) | ((z == 2) & (t <= 1))
    feeder = ((z != t) & (z != 1) & (z != 2)) | ((z == 1) & (t == 0)) | ((z == 2) & (t == 3))
    plane = jnp.where(feeder & (z == 0), 1, jnp.where(feeder & (z == line - 1), 2, t))

    def remote(src, dst, send, recv, device):
        return pltpu.make_async_remote_copy(
            src_ref=src, dst_ref=dst, send_sem=send, recv_sem=recv,
            device_id=device, device_id_type=MESH,
        )

    def g_copy(r, f):
        if r == 3:
            return remote(gbuf.at[2, f], gbuf.at[3, f], g_send.at[3, f], g_recv.at[3, f], partner)
        src = cot_ref.at[:, pl.ds(f * SUB, SUB)]
        return remote(
            src, gbuf.at[r, f], g_send.at[r, f], g_recv.at[r, f], partner if r == 1 else across)

    for f in range(n_ff):
        g_copy(2, f).start()
        g_copy(1, f).start()

    def y_copies(s):
        return (
            remote(y_out.at[s], y_in.at[s], y_send.at[0, s], y_recv.at[0, s], pair),
            remote(y_out_s.at[s], y_in_s.at[s], y_send.at[1, s], y_recv.at[1, s], pair),
        )

    def w_copies(s, way):
        device = (2 * plane + y, t)
        return (
            remote(w_out.at[s], w_in.at[way, s], w_send.at[0, s], w_recv.at[way, 0, s], device),
            remote(w_out_s.at[s], w_in_s.at[way, s], w_send.at[1, s], w_recv.at[way, 1, s], device),
        )

    def place(f, h, e):
        down = pl.ds(h * tall, tall)
        along = pl.ds(pl.multiple_of(f * SUB, SUB), SUB)
        return e, down, along

    def f_copies(s, r, f, h):
        return [
            remote(
                acc.at[s, :, pl.ds(e * SUB, SUB)], result.at[place(f, h, e)],
                f_send.at[s, e], f_recv.at[f, h, e], (d, rel(r)))
            for e in range(experts)
        ]

    def stores(f, h):
        return [
            pltpu.make_async_copy(
                result.at[place(f, h, e)], out_ref.at[place(f, h, e)], store_sem.at[f, h, e])
            for e in range(experts)
        ]

    chunk = 256
    part = tall // 4

    def unscaled(data, scale, at):
        return data[at, :].astype(jnp.int32).astype(jnp.float32) * scale[...]

    def highest(top, value):
        return jnp.maximum(top, jnp.max(jnp.abs(value), axis=0, keepdims=True))

    def put(value, top, data, scale):
        top = jnp.maximum(top, TINY)
        factor = STEPS / top
        scale[...] = top * (1.0 / STEPS)
        for k in range(4):
            at = pl.ds(k * part, part)
            whole = jnp.round(value[at, :] * factor).astype(jnp.int32)
            data[at, :] = whole.astype(jnp.int16)

    def turn(p, h):
        loads[p, h].wait()

        @pl.loop(0, rows // chunk)
        def _(i):
            at = pl.ds(pl.multiple_of(i * chunk, chunk), chunk)
            for b in range(tall // SUB):
                block = xv[p, h, at, b * SUB : (b + 1) * SUB].astype(jnp.float32).T
                xt[p, h, b * SUB : (b + 1) * SUB, at] = block.astype(xt.dtype)

    def arrive(r, f):
        for k in range(n_ff):
            @pl.when((r == 0) & (f == k))
            def _():
                loads[k].wait()

            @pl.when((r == 1) & (f == k))
            def _():
                g_copy(1, k).wait_recv()

            @pl.when((r == 2) & (f == k))
            def _():
                g_copy(2, k).wait_recv()
                g_copy(3, k).start()

            @pl.when((r == 3) & (f == k))
            def _():
                g_copy(3, k).wait_recv()

    def product(p, h, into):
        for e in range(experts):
            deep = rows * (e + 1) // experts
            value = jnp.dot(
                xt[p, h, :, :deep], gm[:deep, 2 * e * SUB : 2 * (e + 1) * SUB],
                preferred_element_type=jnp.float32,
            )
            for a in range(2):
                into[a, :, e * SUB : (e + 1) * SUB] = value[:, a * SUB : (a + 1) * SUB]

    def form(s):
        k, h = s // 4, (s // 2) % 2

        @pl.when(h == 0)
        def _():
            for a in range(2):
                r, f = pick(unit_r, 2 * k + a), pick(unit_f, 2 * k + a)
                arrive(r, f)
                for e in range(experts):
                    low = start_ref[0, e]
                    high = low + length_ref[0, e]

                    @pl.loop(0, rows * (e + 1) // experts // chunk)
                    def _(i):
                        at = pl.ds(pl.multiple_of(i * chunk, chunk), chunk)
                        block = gbuf[r, f, at, :].astype(jnp.float32)
                        row = i * chunk + lax.broadcasted_iota(jnp.int32, (chunk, SUB), 0)
                        keep = (row >= low) & (row < high)
                        gm[at, (2 * e + a) * SUB : (2 * e + a + 1) * SUB] = jnp.where(
                            keep, block, 0.0
                        ).astype(gm.dtype)

        for step in range(2):
            @pl.when(s == 2 * step)
            def _():
                turn(0, step)

        product(0, h, fresh)
        for a in range(2):
            put(fresh.at[a], highest(0.0, fresh[a]), y_out.at[s + a], y_out_s.at[s + a])
            for copy in y_copies(s + a):
                copy.start()

        for step in range(2):
            @pl.when(s == 2 * step)
            def _():
                turn(1, step)

        product(1, h, acc.at[pl.ds(s, 2)])

    def settle(s, sources):
        h = (s // 2) % 2
        r, f = pick(unit_r, unit_of(s)), pick(unit_f, unit_of(s))
        for copy in y_copies(s):
            copy.wait_recv()
        for way in range(sources):
            for copy in w_copies(s, way):
                copy.wait_recv()
        top = jnp.zeros((1, acc.shape[2]), jnp.float32)
        for k in range(4):
            at = pl.ds(k * part, part)
            value = acc[s, at, :] + unscaled(y_in.at[s], y_in_s.at[s], at)
            for way in range(sources):
                value += unscaled(w_in.at[way, s], w_in_s.at[way, s], at)
            acc[s, at, :] = value
            if sources < 2:
                top = highest(top, value)
        if sources < 2:
            put(acc.at[s], top, w_out.at[s], w_out_s.at[s])
            for copy in w_copies(s, sources):
                copy.start()
            return

        @pl.when(r == 0)
        def _():
            for e in range(experts):
                result[place(f, h, e)] = acc[s, :, e * SUB : (e + 1) * SUB]
            for copy in stores(f, h):
                copy.start()

        @pl.when(r != 0)
        def _():
            for copy in f_copies(s, r, f, h):
                copy.start()

    lags = (JOIN, JOIN + MERGE, JOIN + LAST)

    @pl.loop(0, count + lags[2])
    def _(i):
        @pl.when((i < count) & (i % 2 == 0))
        def _():
            form(i)

        for sources, role in enumerate((feeder, merger, target)):
            @pl.when(role & (i >= lags[sources]) & (i < count + lags[sources]))
            def _():
                settle(i - lags[sources], sources)

    blocks = [(f, h) for f in range(n_ff) for h in range(2)]

    @pl.when(z != t)
    def _():
        for f, h in blocks:
            for e, copy in enumerate(f_copies(0, 1, f, h)):
                copy.wait_recv()
            for copy in stores(f, h):
                copy.start()

    @pl.loop(0, count)
    def _(s):
        r = pick(unit_r, unit_of(s))
        for copy in y_copies(s):
            copy.wait_send()

        @pl.when(z != t)
        def _():
            for copy in w_copies(s, 0):
                copy.wait_send()

        @pl.when((z == t) & (r != 0))
        def _():
            for copy in f_copies(s, r, 0, 0):
                copy.wait_send()

    for f in range(n_ff):
        for r in range(1, 4):
            g_copy(r, f).wait_send()
    for f, h in blocks:
        for copy in stores(f, h):
            copy.wait()


def kernel_device(n_dp, n_t, tokens, cotangent, seg_start, seg_length):
    rows, width = tokens.shape
    ff = cotangent.shape[1]
    experts = seg_start.shape[1]
    half = width // 2
    tall = half // 2
    n_ff = ff // SUB
    count = 2 * n_t * n_ff
    wide = experts * SUB
    dma = pltpu.SemaphoreType.DMA
    anywhere = pl.BlockSpec(memory_space=pl.ANY)
    scalars = pl.BlockSpec(memory_space=pltpu.SMEM)
    data = pltpu.VMEM((count, tall, wide), jnp.int16)
    scale = pltpu.VMEM((count, 1, wide), jnp.float32)
    out = pl.pallas_call(
        functools.partial(grad_kernel, n_dp, n_t, experts),
        out_shape=jax.ShapeDtypeStruct((experts, half, ff), jnp.float32),
        in_specs=[anywhere, anywhere, scalars, scalars],
        out_specs=anywhere,
        scratch_shapes=[
            pltpu.VMEM((2, 2, rows, tall), tokens.dtype),
            pltpu.VMEM((2, 2, tall, rows), tokens.dtype),
            pltpu.VMEM((n_t, n_ff, rows, SUB), cotangent.dtype),
            pltpu.VMEM((rows, 2 * wide), cotangent.dtype),
            pltpu.VMEM((count, tall, wide), jnp.float32),
            pltpu.VMEM((2, tall, wide), jnp.float32),
            pltpu.VMEM((experts, half, ff), jnp.float32),
            data, data, data,
            pltpu.VMEM((2, count, tall, wide), jnp.int16),
            scale, scale, scale,
            pltpu.VMEM((2, count, 1, wide), jnp.float32),
            dma((n_ff + 4,)),
            dma((n_t, n_ff)),
            dma((n_t, n_ff)),
            dma((2, count)),
            dma((2, count)),
            dma((2, count)),
            dma((2, 2, count)),
            dma((count, experts)),
            dma((n_ff, 2, experts)),
            dma((n_ff, 2, experts)),
        ],
        compiler_params=pltpu.CompilerParams(
            collective_id=0, has_side_effects=True, vmem_limit_bytes=67043328
        ),
    )(tokens, cotangent, seg_start, seg_length)
    return out.transpose(1, 0, 2)


def solution(mesh):
    n_dp, n_t = mesh.shape["dp"], mesh.shape["tensor"]
    body = plain_device
    if n_t == 4 and n_dp == 2 * n_t:
        body = functools.partial(kernel_device, n_dp, n_t)
    in_specs = (P("dp", "tensor"), P("dp", "tensor"), P("dp", None), P("dp", None))
    out_specs = P("dp", None, "tensor")
    return jax.shard_map(
        body, mesh=mesh, in_specs=in_specs, out_specs=out_specs, check_vma=False
    )
```

```python
import functools

import jax
import jax.numpy as jnp
from jax import lax
from jax.experimental import pallas as pl
from jax.experimental.pallas import tpu as pltpu
from jax.sharding import PartitionSpec as P

CAP = 1024
SUB = 128
STEPS = 32767.0
TINY = 1e-30
JOIN, MERGE, LAST = 2, 2, 5
MESH = pl.DeviceIdType.MESH


def block_term(columns, grads, lower, upper, size):
    total_rows = columns.shape[0]
    first = jnp.minimum(lower, total_rows - size)
    rows = first + jnp.arange(size, dtype=jnp.int32)
    keep = (rows >= lower) & (rows < upper)
    block_x = lax.dynamic_slice_in_dim(columns, first, size, 0)
    block_g = lax.dynamic_slice_in_dim(grads, first, size, 0)
    block_g = jnp.where(keep[:, None], block_g, jnp.zeros_like(block_g))
    return lax.dot_general(
        block_x, block_g, (((0,), (0,)), ((), ())), preferred_element_type=jnp.float32
    )


def plain_device(tokens, cotangent, seg_start, seg_length):
    whole = lax.all_gather(tokens, "tensor", axis=1, tiled=True)
    terms = []
    for expert in range(seg_start.shape[1]):
        start = seg_start[0, expert]
        upper = start + seg_length[0, expert]
        terms.append(block_term(whole, cotangent, start, upper, CAP))
    return lax.psum_scatter(jnp.stack(terms, 1), "dp", scatter_dimension=0, tiled=True)


def unit_order(n_ff):
    if n_ff == 3:
        return [
            (0, 0), (0, 1), (1, 0), (1, 1), (2, 0), (3, 0),
            (2, 1), (3, 1), (2, 2), (3, 2), (1, 2), (0, 2),
        ]
    return [(r, f) for f in range(n_ff) for r in range(4)]


def pick(values, i):
    found = jnp.int32(values[0])
    for k in range(1, len(values)):
        found = jnp.where(i == k, values[k], found)
    return found


def grad_kernel(
    n_dp, n_t, experts, tok_ref, cot_ref, start_ref, length_ref, out_ref,
    xv, xt, gbuf, gm, acc, fresh, result, y_out, y_in, w_out, w_in,
    y_out_s, y_in_s, w_out_s, w_in_s,
    load_sem, g_send, g_recv, y_send, y_recv, w_send, w_recv, f_send, f_recv, store_sem,
):
    d = lax.axis_index("dp")
    t = lax.axis_index("tensor")
    line = n_dp // 2
    z, y = d // 2, d % 2
    x, c = t // 2, t % 2
    rows = cot_ref.shape[0]
    n_ff = gbuf.shape[1]
    tall = xv.shape[3]
    half = 2 * tall
    units = unit_order(n_ff)
    count = 2 * len(units)
    unit_r = [r for r, f in units]
    unit_f = [f for r, f in units]

    def unit_of(s):
        return 2 * (s // 4) + s % 2

    def rel(r):
        return 2 * ((x + r // 2) % 2) + (c + r % 2) % 2

    pair = (d + 1 - 2 * y, t)
    partner, across = (d, rel(1)), (d, rel(2))

    loads = {}
    for f in range(n_ff):
        loads[f] = pltpu.make_async_copy(
            cot_ref.at[:, pl.ds(f * SUB, SUB)], gbuf.at[0, f], load_sem.at[f])
    for p, parity in enumerate((1 - y, y)):
        for h in range(2):
            at = pl.ds(pl.multiple_of(parity * half + h * tall, tall), tall)
            loads[p, h] = pltpu.make_async_copy(
                tok_ref.at[:, at], xv.at[p, h], load_sem.at[n_ff + 2 * p + h])
    for name in [(0, 0), 0, 1, (1, 0), (0, 1), (1, 1)] + list(range(2, n_ff)):
        loads[name].start()

    barrier = pltpu.get_barrier_semaphore()
    others = [(2 * ((z + k) % line) + y, t) for k in range(1, line)]
    for device in [pair] + [(d, rel(r)) for r in range(1, 4)] + others:
        pl.semaphore_signal(barrier, inc=1, device_id=device, device_id_type=MESH)

    target = z == t
    merger = ((z == 1) & (t >= 2)) | ((z == 2) & (t <= 1))
    feeder = ((z != t) & (z != 1) & (z != 2)) | ((z == 1) & (t == 0)) | ((z == 2) & (t == 3))
    plane = jnp.where(feeder & (z == 0), 1, jnp.where(feeder & (z == line - 1), 2, t))

    def remote(src, dst, send, recv, device):
        return pltpu.make_async_remote_copy(
            src_ref=src, dst_ref=dst, send_sem=send, recv_sem=recv,
            device_id=device, device_id_type=MESH,
        )

    def g_copy(r, f):
        if r == 3:
            return remote(gbuf.at[2, f], gbuf.at[3, f], g_send.at[3, f], g_recv.at[3, f], partner)
        src = cot_ref.at[:, pl.ds(f * SUB, SUB)]
        return remote(
            src, gbuf.at[r, f], g_send.at[r, f], g_recv.at[r, f], partner if r == 1 else across)

    def y_copies(s):
        return (
            remote(y_out.at[s], y_in.at[s], y_send.at[0, s], y_recv.at[0, s], pair),
            remote(y_out_s.at[s], y_in_s.at[s], y_send.at[1, s], y_recv.at[1, s], pair),
        )

    def w_copies(s, way):
        device = (2 * plane + y, t)
        return (
            remote(w_out.at[s], w_in.at[way, s], w_send.at[0, s], w_recv.at[way, 0, s], device),
            remote(w_out_s.at[s], w_in_s.at[way, s], w_send.at[1, s], w_recv.at[way, 1, s], device),
        )

    def place(f, h, e):
        down = pl.ds(h * tall, tall)
        along = pl.ds(pl.multiple_of(f * SUB, SUB), SUB)
        return e, down, along

    def f_copies(s, r, f, h):
        return [
            remote(
                acc.at[s, :, pl.ds(e * SUB, SUB)], result.at[place(f, h, e)],
                f_send.at[s, e], f_recv.at[f, h, e], (d, rel(r)))
            for e in range(experts)
        ]

    def stores(f, h):
        return [
            pltpu.make_async_copy(
                result.at[place(f, h, e)], out_ref.at[place(f, h, e)], store_sem.at[f, h, e])
            for e in range(experts)
        ]

    chunk = 256
    part = tall // 4

    def unscaled(data, scale, at):
        return data[at, :].astype(jnp.int32).astype(jnp.float32) * scale[...]

    def highest(top, value):
        return jnp.maximum(top, jnp.max(jnp.abs(value), axis=0, keepdims=True))

    def put(value, top, data, scale):
        top = jnp.maximum(top, TINY)
        factor = STEPS / top
        scale[...] = top * (1.0 / STEPS)
        for k in range(4):
            at = pl.ds(k * part, part)
            whole = jnp.round(value[at, :] * factor).astype(jnp.int32)
            data[at, :] = whole.astype(jnp.int16)

    def turn(p, h):
        loads[p, h].wait()

        @pl.loop(0, rows // chunk)
        def _(i):
            at = pl.ds(pl.multiple_of(i * chunk, chunk), chunk)
            for b in range(tall // SUB):
                block = xv[p, h, at, b * SUB : (b + 1) * SUB].T
                xt[p, h, b * SUB : (b + 1) * SUB, at] = block.astype(xt.dtype)

    def arrive(r, f):
        for k in range(n_ff):
            @pl.when((r == 0) & (f == k))
            def _():
                loads[k].wait()

            @pl.when((r == 1) & (f == k))
            def _():
                g_copy(1, k).wait_recv()

            @pl.when((r == 2) & (f == k))
            def _():
                g_copy(2, k).wait_recv()
                g_copy(3, k).start()

            @pl.when((r == 3) & (f == k))
            def _():
                g_copy(3, k).wait_recv()

    def product(p, h, into):
        for e in range(experts):
            deep = rows * (e + 1) // experts
            value = jnp.dot(
                xt[p, h, :, :deep], gm[:deep, 2 * e * SUB : 2 * (e + 1) * SUB],
                preferred_element_type=jnp.float32,
            )
            for a in range(2):
                into[a, :, e * SUB : (e + 1) * SUB] = value[:, a * SUB : (a + 1) * SUB]

    def cover(r, f, a):
        for e in range(experts):
            low = start_ref[0, e]
            high = low + length_ref[0, e]

            @pl.loop(0, rows * (e + 1) // experts // chunk)
            def _(i):
                at = pl.ds(pl.multiple_of(i * chunk, chunk), chunk)
                block = gbuf[r, f, at, :].astype(jnp.float32)
                row = i * chunk + lax.broadcasted_iota(jnp.int32, (chunk, SUB), 0)
                keep = (row >= low) & (row < high)
                gm[at, (2 * e + a) * SUB : (2 * e + a + 1) * SUB] = jnp.where(
                    keep, block, 0.0
                ).astype(gm.dtype)

    def ready(s, h):
        product(0, h, fresh)
        for a in range(2):
            put(fresh.at[a], highest(0.0, fresh[a]), y_out.at[s + a], y_out_s.at[s + a])

    def form(s):
        k, h = s // 4, (s // 2) % 2

        @pl.when((h == 0) & (s > 0))
        def _():
            for a in range(2):
                r, f = pick(unit_r, 2 * k + a), pick(unit_f, 2 * k + a)
                arrive(r, f)
                cover(r, f, a)

        @pl.when(s == 2)
        def _():
            turn(0, 1)

        @pl.when(s > 0)
        def _():
            ready(s, h)

        for a in range(2):
            for copy in y_copies(s + a):
                copy.start()

        for step in range(2):
            @pl.when(s == 2 * step)
            def _():
                turn(1, step)

        product(1, h, acc.at[pl.ds(s, 2)])

    def settle(s, sources):
        h = (s // 2) % 2
        r, f = pick(unit_r, unit_of(s)), pick(unit_f, unit_of(s))
        for copy in y_copies(s):
            copy.wait_recv()
        for way in range(sources):
            for copy in w_copies(s, way):
                copy.wait_recv()
        top = jnp.zeros((1, acc.shape[2]), jnp.float32)
        for k in range(4):
            at = pl.ds(k * part, part)
            value = acc[s, at, :] + unscaled(y_in.at[s], y_in_s.at[s], at)
            for way in range(sources):
                value += unscaled(w_in.at[way, s], w_in_s.at[way, s], at)
            acc[s, at, :] = value
            if sources < 2:
                top = highest(top, value)
        if sources < 2:
            put(acc.at[s], top, w_out.at[s], w_out_s.at[s])
            for copy in w_copies(s, sources):
                copy.start()
            return

        @pl.when(r == 0)
        def _():
            for e in range(experts):
                result[place(f, h, e)] = acc[s, :, e * SUB : (e + 1) * SUB]
            for copy in stores(f, h):
                copy.start()

        @pl.when(r != 0)
        def _():
            for copy in f_copies(s, r, f, h):
                copy.start()

    turn(0, 0)
    for a in range(2):
        loads[units[a][1]].wait()
        cover(*units[a], a)
    ready(0, 0)
    pl.semaphore_wait(barrier, 4 + len(others))
    for f in range(n_ff):
        g_copy(2, f).start()
        g_copy(1, f).start()

    lags = (JOIN, JOIN + MERGE, JOIN + LAST)

    @pl.loop(0, count + lags[2])
    def _(i):
        @pl.when((i < count) & (i % 2 == 0))
        def _():
            form(i)

        for sources, role in enumerate((feeder, merger, target)):
            @pl.when(role & (i >= lags[sources]) & (i < count + lags[sources]))
            def _():
                settle(i - lags[sources], sources)

    blocks = [(f, h) for f in range(n_ff) for h in range(2)]

    @pl.when(z != t)
    def _():
        for f, h in blocks:
            for e, copy in enumerate(f_copies(0, 1, f, h)):
                copy.wait_recv()
            for copy in stores(f, h):
                copy.start()

    @pl.loop(0, count)
    def _(s):
        r = pick(unit_r, unit_of(s))
        for copy in y_copies(s):
            copy.wait_send()

        @pl.when(z != t)
        def _():
            for copy in w_copies(s, 0):
                copy.wait_send()

        @pl.when((z == t) & (r != 0))
        def _():
            for copy in f_copies(s, r, 0, 0):
                copy.wait_send()

    for f in range(n_ff):
        for r in range(1, 4):
            g_copy(r, f).wait_send()
    for f, h in blocks:
        for copy in stores(f, h):
            copy.wait()


def kernel_device(n_dp, n_t, tokens, cotangent, seg_start, seg_length):
    rows, width = tokens.shape
    ff = cotangent.shape[1]
    experts = seg_start.shape[1]
    half = width // 2
    tall = half // 2
    n_ff = ff // SUB
    count = 2 * n_t * n_ff
    wide = experts * SUB
    dma = pltpu.SemaphoreType.DMA
    anywhere = pl.BlockSpec(memory_space=pl.ANY)
    scalars = pl.BlockSpec(memory_space=pltpu.SMEM)
    data = pltpu.VMEM((count, tall, wide), jnp.int16)
    scale = pltpu.VMEM((count, 1, wide), jnp.float32)
    out = pl.pallas_call(
        functools.partial(grad_kernel, n_dp, n_t, experts),
        out_shape=jax.ShapeDtypeStruct((experts, half, ff), jnp.float32),
        in_specs=[anywhere, anywhere, scalars, scalars],
        out_specs=anywhere,
        scratch_shapes=[
            pltpu.VMEM((2, 2, rows, tall), tokens.dtype),
            pltpu.VMEM((2, 2, tall, rows), tokens.dtype),
            pltpu.VMEM((n_t, n_ff, rows, SUB), cotangent.dtype),
            pltpu.VMEM((rows, 2 * wide), cotangent.dtype),
            pltpu.VMEM((count, tall, wide), jnp.float32),
            pltpu.VMEM((2, tall, wide), jnp.float32),
            pltpu.VMEM((experts, half, ff), jnp.float32),
            data, data, data,
            pltpu.VMEM((2, count, tall, wide), jnp.int16),
            scale, scale, scale,
            pltpu.VMEM((2, count, 1, wide), jnp.float32),
            dma((n_ff + 4,)),
            dma((n_t, n_ff)),
            dma((n_t, n_ff)),
            dma((2, count)),
            dma((2, count)),
            dma((2, count)),
            dma((2, 2, count)),
            dma((count, experts)),
            dma((n_ff, 2, experts)),
            dma((n_ff, 2, experts)),
        ],
        compiler_params=pltpu.CompilerParams(
            collective_id=0, has_side_effects=True, vmem_limit_bytes=67043328
        ),
    )(tokens, cotangent, seg_start, seg_length)
    return out.transpose(1, 0, 2)


def solution(mesh):
    n_dp, n_t = mesh.shape["dp"], mesh.shape["tensor"]
    body = plain_device
    if n_t == 4 and n_dp == 2 * n_t:
        body = functools.partial(kernel_device, n_dp, n_t)
    in_specs = (P("dp", "tensor"), P("dp", "tensor"), P("dp", None), P("dp", None))
    out_specs = P("dp", None, "tensor")
    return jax.shard_map(
        body, mesh=mesh, in_specs=in_specs, out_specs=out_specs, check_vma=False
    )
```

```python
import functools

import jax
import jax.numpy as jnp
from jax import lax
from jax.experimental import pallas as pl
from jax.experimental.pallas import tpu as pltpu
from jax.sharding import PartitionSpec as P

CAP = 1024
SUB = 128
STEPS = 32767.0
TINY = 1e-30
JOIN, MERGE, LAST = 4, 1, 3
MESH = pl.DeviceIdType.MESH


def block_term(columns, grads, lower, upper, size):
    total_rows = columns.shape[0]
    first = jnp.minimum(lower, total_rows - size)
    rows = first + jnp.arange(size, dtype=jnp.int32)
    keep = (rows >= lower) & (rows < upper)
    block_x = lax.dynamic_slice_in_dim(columns, first, size, 0)
    block_g = lax.dynamic_slice_in_dim(grads, first, size, 0)
    block_g = jnp.where(keep[:, None], block_g, jnp.zeros_like(block_g))
    return lax.dot_general(
        block_x, block_g, (((0,), (0,)), ((), ())), preferred_element_type=jnp.float32
    )


def plain_device(tokens, cotangent, seg_start, seg_length):
    whole = lax.all_gather(tokens, "tensor", axis=1, tiled=True)
    terms = []
    for expert in range(seg_start.shape[1]):
        start = seg_start[0, expert]
        upper = start + seg_length[0, expert]
        terms.append(block_term(whole, cotangent, start, upper, CAP))
    return lax.psum_scatter(jnp.stack(terms, 1), "dp", scatter_dimension=0, tiled=True)


def unit_order(n_ff):
    if n_ff == 3:
        return [
            (0, 0), (0, 1), (1, 0), (1, 1), (2, 0), (3, 0),
            (2, 1), (3, 1), (2, 2), (3, 2), (1, 2), (0, 2),
        ]
    return [(r, f) for f in range(n_ff) for r in range(4)]


def pick(values, i):
    found = jnp.int32(values[0])
    for k in range(1, len(values)):
        found = jnp.where(i == k, values[k], found)
    return found


def grad_kernel(
    n_dp, n_t, experts, tok_ref, cot_ref, start_hbm, length_hbm, out_ref,
    xv, xt, gbuf, gm, acc, fresh, result, y_out, y_in, w_out, w_in,
    y_out_s, y_in_s, w_out_s, w_in_s,
    load_sem, g_send, g_recv, y_send, y_recv, w_send, w_recv, f_send, f_recv, store_sem,
    start_ref, length_ref, seg_sem,
):
    d = lax.axis_index("dp")
    t = lax.axis_index("tensor")
    line = n_dp // 2
    z, y = d // 2, d % 2
    x, c = t // 2, t % 2
    rows = cot_ref.shape[0]
    n_ff = gbuf.shape[1]
    tall = xv.shape[3]
    half = 2 * tall
    units = unit_order(n_ff)
    count = 2 * len(units)
    unit_r = [r for r, f in units]
    unit_f = [f for r, f in units]

    def unit_of(s):
        return 2 * (s // 4) + s % 2

    def rel(r):
        return 2 * ((x + r // 2) % 2) + (c + r % 2) % 2

    pair = (d + 1 - 2 * y, t)
    partner, across = (d, rel(1)), (d, rel(2))

    loads = {}
    for f in range(n_ff):
        loads[f] = pltpu.make_async_copy(
            cot_ref.at[:, pl.ds(f * SUB, SUB)], gbuf.at[0, f], load_sem.at[f])
    for p, parity in enumerate((1 - y, y)):
        for h in range(2):
            at = pl.ds(pl.multiple_of(parity * half + h * tall, tall), tall)
            loads[p, h] = pltpu.make_async_copy(
                tok_ref.at[:, at], xv.at[p, h], load_sem.at[n_ff + 2 * p + h])
    for name in [(0, 0), 0, 1, (1, 0), (0, 1), (1, 1)] + list(range(2, n_ff)):
        loads[name].start()
    segments = [
        pltpu.make_async_copy(start_hbm, start_ref, seg_sem.at[0]),
        pltpu.make_async_copy(length_hbm, length_ref, seg_sem.at[1]),
    ]
    for copy in segments:
        copy.start()

    barrier = pltpu.get_barrier_semaphore()
    others = [(2 * ((z + k) % line) + y, t) for k in range(1, line)]
    for device in [pair] + [(d, rel(r)) for r in range(1, 4)] + others:
        pl.semaphore_signal(barrier, inc=1, device_id=device, device_id_type=MESH)

    target = z == t
    merger = ((z == 1) & (t >= 2)) | ((z == 2) & (t <= 1))
    feeder = ((z != t) & (z != 1) & (z != 2)) | ((z == 1) & (t == 0)) | ((z == 2) & (t == 3))
    plane = jnp.where(feeder & (z == 0), 1, jnp.where(feeder & (z == line - 1), 2, t))

    def remote(src, dst, send, recv, device):
        return pltpu.make_async_remote_copy(
            src_ref=src, dst_ref=dst, send_sem=send, recv_sem=recv,
            device_id=device, device_id_type=MESH,
        )

    def g_copy(r, f):
        if r == 3:
            return remote(gbuf.at[2, f], gbuf.at[3, f], g_send.at[3, f], g_recv.at[3, f], partner)
        src = cot_ref.at[:, pl.ds(f * SUB, SUB)]
        return remote(
            src, gbuf.at[r, f], g_send.at[r, f], g_recv.at[r, f], partner if r == 1 else across)

    def y_copy(s):
        return remote(y_out.at[s], y_in.at[s], y_send.at[0, s], y_recv.at[0, s], pair)

    def y_scale(s):
        at = pl.ds(s, 2)
        return remote(y_out_s.at[at], y_in_s.at[at], y_send.at[1, s], y_recv.at[1, s], pair)

    def w_copies(s, way):
        device = (2 * plane + y, t)
        return (
            remote(w_out.at[s], w_in.at[way, s], w_send.at[0, s], w_recv.at[way, 0, s], device),
            remote(w_out_s.at[s], w_in_s.at[way, s], w_send.at[1, s], w_recv.at[way, 1, s], device),
        )

    def place(f, h, e):
        down = pl.ds(h * tall, tall)
        along = pl.ds(pl.multiple_of(f * SUB, SUB), SUB)
        return e, down, along

    def f_copies(s, r, f, h):
        return [
            remote(
                acc.at[s, :, pl.ds(e * SUB, SUB)], result.at[place(f, h, e)],
                f_send.at[s, e], f_recv.at[f, h, e], (d, rel(r)))
            for e in range(experts)
        ]

    def stores(f, h):
        return [
            pltpu.make_async_copy(
                result.at[place(f, h, e)], out_ref.at[place(f, h, e)], store_sem.at[f, h, e])
            for e in range(experts)
        ]

    chunk = 256
    part = tall // 4

    def unscaled(data, scale, at):
        return data[at, :].astype(jnp.int32).astype(jnp.float32) * scale[...]

    def highest(top, value):
        return jnp.maximum(top, jnp.max(jnp.abs(value), axis=0, keepdims=True))

    def put(value, top, data, scale):
        top = jnp.maximum(top, TINY)
        factor = STEPS / top
        scale[...] = top * (1.0 / STEPS)
        for k in range(4):
            at = pl.ds(k * part, part)
            whole = jnp.round(value[at, :] * factor).astype(jnp.int32)
            data[at, :] = whole.astype(jnp.int16)

    def turn(p, h):
        loads[p, h].wait()

        @pl.loop(0, rows // chunk)
        def _(i):
            at = pl.ds(pl.multiple_of(i * chunk, chunk), chunk)
            for b in range(tall // SUB):
                block = xv[p, h, at, b * SUB : (b + 1) * SUB].T
                xt[p, h, b * SUB : (b + 1) * SUB, at] = block.astype(xt.dtype)

    def arrive(r, f):
        for k in range(n_ff):
            @pl.when((r == 0) & (f == k))
            def _():
                loads[k].wait()

            @pl.when((r == 1) & (f == k))
            def _():
                g_copy(1, k).wait_recv()

            @pl.when((r == 2) & (f == k))
            def _():
                g_copy(2, k).wait_recv()
                g_copy(3, k).start()

            @pl.when((r == 3) & (f == k))
            def _():
                g_copy(3, k).wait_recv()

    def product(p, h, into):
        for e in range(experts):
            deep = rows * (e + 1) // experts
            value = jnp.dot(
                xt[p, h, :, :deep], gm[:deep, 2 * e * SUB : 2 * (e + 1) * SUB],
                preferred_element_type=jnp.float32,
            )
            for a in range(2):
                into[a, :, e * SUB : (e + 1) * SUB] = value[:, a * SUB : (a + 1) * SUB]

    def cover(r, f, a):
        for e in range(experts):
            low = start_ref[0, e]
            high = low + length_ref[0, e]

            @pl.loop(0, rows * (e + 1) // experts // chunk)
            def _(i):
                at = pl.ds(pl.multiple_of(i * chunk, chunk), chunk)
                block = gbuf[r, f, at, :].astype(jnp.float32)
                row = i * chunk + lax.broadcasted_iota(jnp.int32, (chunk, SUB), 0)
                keep = (row >= low) & (row < high)
                gm[at, (2 * e + a) * SUB : (2 * e + a + 1) * SUB] = jnp.where(
                    keep, block, 0.0
                ).astype(gm.dtype)

    def ready(s, h):
        product(0, h, fresh)
        for a in range(2):
            put(fresh.at[a], highest(0.0, fresh[a]), y_out.at[s + a], y_out_s.at[s + a])

    def form(s):
        k, h = s // 4, (s // 2) % 2

        @pl.when((h == 0) & (s > 0))
        def _():
            for a in range(2):
                r, f = pick(unit_r, 2 * k + a), pick(unit_f, 2 * k + a)
                arrive(r, f)
                cover(r, f, a)

        @pl.when(s == 2)
        def _():
            turn(0, 1)

        @pl.when(s > 0)
        def _():
            ready(s, h)

        y_scale(s).start()
        for a in range(2):
            y_copy(s + a).start()

    def keep_half(s):
        h = (s // 2) % 2
        for step in range(2):
            @pl.when(s == 2 * step)
            def _():
                turn(1, step)

        product(1, h, acc.at[pl.ds(s, 2)])

    def settle(s, sources):
        h = (s // 2) % 2
        r, f = pick(unit_r, unit_of(s)), pick(unit_f, unit_of(s))
        y_copy(s).wait_recv()

        @pl.when(s % 2 == 0)
        def _():
            y_scale(s).wait_recv()

        for way in range(sources):
            for copy in w_copies(s, way):
                copy.wait_recv()
        top = jnp.zeros((1, acc.shape[2]), jnp.float32)
        for k in range(4):
            at = pl.ds(k * part, part)
            value = acc[s, at, :] + unscaled(y_in.at[s], y_in_s.at[s], at)
            for way in range(sources):
                value += unscaled(w_in.at[way, s], w_in_s.at[way, s], at)
            acc[s, at, :] = value
            if sources < 2:
                top = highest(top, value)
        if sources < 2:
            put(acc.at[s], top, w_out.at[s], w_out_s.at[s])
            for copy in w_copies(s, sources):
                copy.start()
            return

        @pl.when(r == 0)
        def _():
            for e in range(experts):
                result[place(f, h, e)] = acc[s, :, e * SUB : (e + 1) * SUB]
            for copy in stores(f, h):
                copy.start()

        @pl.when(r != 0)
        def _():
            for copy in f_copies(s, r, f, h):
                copy.start()

    turn(0, 0)
    for copy in segments:
        copy.wait()
    for a in range(2):
        loads[units[a][1]].wait()
        cover(*units[a], a)
    ready(0, 0)
    pl.semaphore_wait(barrier, 4 + len(others))
    for f in range(n_ff):
        g_copy(2, f).start()
        g_copy(1, f).start()

    lags = (JOIN, JOIN + MERGE, JOIN + LAST)

    @pl.loop(0, count + lags[2])
    def _(i):
        for sources, role in enumerate((feeder, merger, target)):
            @pl.when(role & (i >= lags[sources]) & (i < count + lags[sources]))
            def _():
                settle(i - lags[sources], sources)

        @pl.when((i < count) & (i % 2 == 0))
        def _():
            form(i)

        @pl.when((i < count) & (i % 2 == 1))
        def _():
            keep_half(i - 1)

    blocks = [(f, h) for f in range(n_ff) for h in range(2)]

    @pl.when(z != t)
    def _():
        for f, h in blocks:
            for e, copy in enumerate(f_copies(0, 1, f, h)):
                copy.wait_recv()
            for copy in stores(f, h):
                copy.start()

    @pl.loop(0, count)
    def _(s):
        r = pick(unit_r, unit_of(s))
        y_copy(s).wait_send()

        @pl.when(s % 2 == 0)
        def _():
            y_scale(s).wait_send()

        @pl.when(z != t)
        def _():
            for copy in w_copies(s, 0):
                copy.wait_send()

        @pl.when((z == t) & (r != 0))
        def _():
            for copy in f_copies(s, r, 0, 0):
                copy.wait_send()

    for f in range(n_ff):
        for r in range(1, 4):
            g_copy(r, f).wait_send()
    for f, h in blocks:
        for copy in stores(f, h):
            copy.wait()


def kernel_device(n_dp, n_t, tokens, cotangent, seg_start, seg_length):
    rows, width = tokens.shape
    ff = cotangent.shape[1]
    experts = seg_start.shape[1]
    half = width // 2
    tall = half // 2
    n_ff = ff // SUB
    count = 2 * n_t * n_ff
    wide = experts * SUB
    dma = pltpu.SemaphoreType.DMA
    anywhere = pl.BlockSpec(memory_space=pl.ANY)
    data = pltpu.VMEM((count, tall, wide), jnp.int16)
    scale = pltpu.VMEM((count, 1, wide), jnp.float32)
    out = pl.pallas_call(
        functools.partial(grad_kernel, n_dp, n_t, experts),
        out_shape=jax.ShapeDtypeStruct((experts, half, ff), jnp.float32),
        in_specs=[anywhere] * 4,
        out_specs=anywhere,
        scratch_shapes=[
            pltpu.VMEM((2, 2, rows, tall), tokens.dtype),
            pltpu.VMEM((2, 2, tall, rows), tokens.dtype),
            pltpu.VMEM((n_t, n_ff, rows, SUB), cotangent.dtype),
            pltpu.VMEM((rows, 2 * wide), cotangent.dtype),
            pltpu.VMEM((count, tall, wide), jnp.float32),
            pltpu.VMEM((2, tall, wide), jnp.float32),
            pltpu.VMEM((experts, half, ff), jnp.float32),
            data, data, data,
            pltpu.VMEM((2, count, tall, wide), jnp.int16),
            scale, scale, scale,
            pltpu.VMEM((2, count, 1, wide), jnp.float32),
            dma((n_ff + 4,)),
            dma((n_t, n_ff)),
            dma((n_t, n_ff)),
            dma((2, count)),
            dma((2, count)),
            dma((2, count)),
            dma((2, 2, count)),
            dma((count, experts)),
            dma((n_ff, 2, experts)),
            dma((n_ff, 2, experts)),
            pltpu.SMEM(seg_start.shape, jnp.int32),
            pltpu.SMEM(seg_length.shape, jnp.int32),
            dma((2,)),
        ],
        compiler_params=pltpu.CompilerParams(
            collective_id=0, has_side_effects=True, vmem_limit_bytes=67043328
        ),
    )(tokens, cotangent, seg_start, seg_length)
    return out.transpose(1, 0, 2)


def solution(mesh):
    n_dp, n_t = mesh.shape["dp"], mesh.shape["tensor"]
    body = plain_device
    if n_t == 4 and n_dp == 2 * n_t:
        body = functools.partial(kernel_device, n_dp, n_t)
    in_specs = (P("dp", "tensor"), P("dp", "tensor"), P("dp", None), P("dp", None))
    out_specs = P("dp", None, "tensor")
    return jax.shard_map(
        body, mesh=mesh, in_specs=in_specs, out_specs=out_specs, check_vma=False
    )
```

```python
import functools

import jax
import jax.numpy as jnp
from jax import lax
from jax.experimental import pallas as pl
from jax.experimental.pallas import tpu as pltpu
from jax.sharding import PartitionSpec as P

CAP = 1024
SUB = 128
STEPS = 32767.0
TINY = 1e-30
JOIN, MERGE, LAST = 4, 1, 2
MESH = pl.DeviceIdType.MESH


def block_term(columns, grads, lower, upper, size):
    total_rows = columns.shape[0]
    first = jnp.minimum(lower, total_rows - size)
    rows = first + jnp.arange(size, dtype=jnp.int32)
    keep = (rows >= lower) & (rows < upper)
    block_x = lax.dynamic_slice_in_dim(columns, first, size, 0)
    block_g = lax.dynamic_slice_in_dim(grads, first, size, 0)
    block_g = jnp.where(keep[:, None], block_g, jnp.zeros_like(block_g))
    return lax.dot_general(
        block_x, block_g, (((0,), (0,)), ((), ())), preferred_element_type=jnp.float32
    )


def plain_device(tokens, cotangent, seg_start, seg_length):
    whole = lax.all_gather(tokens, "tensor", axis=1, tiled=True)
    terms = []
    for expert in range(seg_start.shape[1]):
        start = seg_start[0, expert]
        upper = start + seg_length[0, expert]
        terms.append(block_term(whole, cotangent, start, upper, CAP))
    return lax.psum_scatter(jnp.stack(terms, 1), "dp", scatter_dimension=0, tiled=True)


def unit_order(n_ff):
    if n_ff == 3:
        return [
            (0, 0), (0, 1), (1, 0), (1, 1), (2, 0), (3, 0),
            (2, 1), (3, 1), (2, 2), (3, 2), (1, 2), (0, 2),
        ]
    return [(r, f) for f in range(n_ff) for r in range(4)]


def pick(values, i):
    found = jnp.int32(values[0])
    for k in range(1, len(values)):
        found = jnp.where(i == k, values[k], found)
    return found


def grad_kernel(
    n_dp, n_t, experts, tok_ref, cot_ref, start_hbm, length_hbm, out_ref,
    xv, xt, gbuf, gm, acc, fresh, result, y_out, y_in, w_out, w_in,
    y_out_s, y_in_s, w_out_s, w_in_s,
    load_sem, g_send, g_recv, y_send, y_recv, w_send, w_recv, f_send, f_recv, store_sem,
    start_ref, length_ref, seg_sem,
):
    d = lax.axis_index("dp")
    t = lax.axis_index("tensor")
    line = n_dp // 2
    z, y = d // 2, d % 2
    x, c = t // 2, t % 2
    rows = cot_ref.shape[0]
    n_ff = gbuf.shape[1]
    tall = xv.shape[3]
    half = 2 * tall
    units = unit_order(n_ff)
    count = 2 * len(units)
    unit_r = [r for r, f in units]
    unit_f = [f for r, f in units]

    def unit_of(s):
        return 2 * (s // 4) + s % 2

    def rel(r):
        return 2 * ((x + r // 2) % 2) + (c + r % 2) % 2

    pair = (d + 1 - 2 * y, t)
    partner, across = (d, rel(1)), (d, rel(2))

    loads = {}
    for f in range(n_ff):
        loads[f] = pltpu.make_async_copy(
            cot_ref.at[:, pl.ds(f * SUB, SUB)], gbuf.at[0, f], load_sem.at[f])
    for p, parity in enumerate((1 - y, y)):
        for h in range(2):
            at = pl.ds(pl.multiple_of(parity * half + h * tall, tall), tall)
            loads[p, h] = pltpu.make_async_copy(
                tok_ref.at[:, at], xv.at[p, h], load_sem.at[n_ff + 2 * p + h])
    for name in [(0, 0), 0, 1, (1, 0), (0, 1), (1, 1)] + list(range(2, n_ff)):
        loads[name].start()
    segments = [
        pltpu.make_async_copy(start_hbm, start_ref, seg_sem.at[0]),
        pltpu.make_async_copy(length_hbm, length_ref, seg_sem.at[1]),
    ]
    for copy in segments:
        copy.start()

    barrier = pltpu.get_barrier_semaphore()
    others = [(2 * ((z + k) % line) + y, t) for k in range(1, line)]
    for device in [pair] + [(d, rel(r)) for r in range(1, 4)] + others:
        pl.semaphore_signal(barrier, inc=1, device_id=device, device_id_type=MESH)

    target = z == t
    merger = ((z == 1) & (t >= 2)) | ((z == 2) & (t <= 1))
    feeder = ((z != t) & (z != 1) & (z != 2)) | ((z == 1) & (t == 0)) | ((z == 2) & (t == 3))
    plane = jnp.where(feeder & (z == 0), 1, jnp.where(feeder & (z == line - 1), 2, t))

    def remote(src, dst, send, recv, device):
        return pltpu.make_async_remote_copy(
            src_ref=src, dst_ref=dst, send_sem=send, recv_sem=recv,
            device_id=device, device_id_type=MESH,
        )

    def g_copy(r, f):
        if r == 3:
            return remote(gbuf.at[2, f], gbuf.at[3, f], g_send.at[3, f], g_recv.at[3, f], partner)
        src = cot_ref.at[:, pl.ds(f * SUB, SUB)]
        return remote(
            src, gbuf.at[r, f], g_send.at[r, f], g_recv.at[r, f], partner if r == 1 else across)

    def y_copy(s):
        return remote(y_out.at[s], y_in.at[s], y_send.at[0, s], y_recv.at[0, s], pair)

    def y_scale(s):
        at = pl.ds(s, 2)
        return remote(y_out_s.at[at], y_in_s.at[at], y_send.at[1, s], y_recv.at[1, s], pair)

    def w_copies(s, way):
        device = (2 * plane + y, t)
        return (
            remote(w_out.at[s], w_in.at[way, s], w_send.at[0, s], w_recv.at[way, 0, s], device),
            remote(w_out_s.at[s], w_in_s.at[way, s], w_send.at[1, s], w_recv.at[way, 1, s], device),
        )

    def place(f, h, e):
        down = pl.ds(h * tall, tall)
        along = pl.ds(pl.multiple_of(f * SUB, SUB), SUB)
        return e, down, along

    def f_copies(s, r, f, h):
        return [
            remote(
                acc.at[s, :, pl.ds(e * SUB, SUB)], result.at[place(f, h, e)],
                f_send.at[s, e], f_recv.at[f, h, e], (d, rel(r)))
            for e in range(experts)
        ]

    def stores(f, h):
        return [
            pltpu.make_async_copy(
                result.at[place(f, h, e)], out_ref.at[place(f, h, e)], store_sem.at[f, h, e])
            for e in range(experts)
        ]

    chunk = 256
    part = tall // 4

    def unscaled(data, scale, at):
        return data[at, :].astype(jnp.int32).astype(jnp.float32) * scale[...]

    def highest(top, value):
        return jnp.maximum(top, jnp.max(jnp.abs(value), axis=0, keepdims=True))

    def put(value, top, data, scale):
        top = jnp.maximum(top, TINY)
        factor = STEPS / top
        scale[...] = top * (1.0 / STEPS)
        for k in range(4):
            at = pl.ds(k * part, part)
            whole = jnp.round(value[at, :] * factor).astype(jnp.int32)
            data[at, :] = whole.astype(jnp.int16)

    def turn(p, h):
        loads[p, h].wait()

        @pl.loop(0, rows // chunk)
        def _(i):
            at = pl.ds(pl.multiple_of(i * chunk, chunk), chunk)
            for b in range(tall // SUB):
                block = xv[p, h, at, b * SUB : (b + 1) * SUB].T
                xt[p, h, b * SUB : (b + 1) * SUB, at] = block.astype(xt.dtype)

    def arrive(r, f):
        for k in range(n_ff):
            @pl.when((r == 0) & (f == k))
            def _():
                loads[k].wait()

            @pl.when((r == 1) & (f == k))
            def _():
                g_copy(1, k).wait_recv()

            @pl.when((r == 2) & (f == k))
            def _():
                g_copy(2, k).wait_recv()
                g_copy(3, k).start()

            @pl.when((r == 3) & (f == k))
            def _():
                g_copy(3, k).wait_recv()

    def product(p, h, into):
        for e in range(experts):
            deep = rows * (e + 1) // experts
            value = jnp.dot(
                xt[p, h, :, :deep], gm[:deep, 2 * e * SUB : 2 * (e + 1) * SUB],
                preferred_element_type=jnp.float32,
            )
            for a in range(2):
                into[a, :, e * SUB : (e + 1) * SUB] = value[:, a * SUB : (a + 1) * SUB]

    def cover(r, f, a):
        for e in range(experts):
            low = start_ref[0, e]
            high = low + length_ref[0, e]

            @pl.loop(0, rows * (e + 1) // experts // chunk)
            def _(i):
                at = pl.ds(pl.multiple_of(i * chunk, chunk), chunk)
                block = gbuf[r, f, at, :].astype(jnp.float32)
                row = i * chunk + lax.broadcasted_iota(jnp.int32, (chunk, SUB), 0)
                keep = (row >= low) & (row < high)
                gm[at, (2 * e + a) * SUB : (2 * e + a + 1) * SUB] = jnp.where(
                    keep, block, 0.0
                ).astype(gm.dtype)

    def ready(s, h):
        product(0, h, fresh)
        for a in range(2):
            put(fresh.at[a], highest(0.0, fresh[a]), y_out.at[s + a], y_out_s.at[s + a])

    def form(s):
        k, h = s // 4, (s // 2) % 2

        @pl.when((h == 0) & (s > 0))
        def _():
            for a in range(2):
                r, f = pick(unit_r, 2 * k + a), pick(unit_f, 2 * k + a)
                arrive(r, f)
                cover(r, f, a)

        @pl.when(s == 2)
        def _():
            turn(0, 1)

        @pl.when(s > 0)
        def _():
            ready(s, h)

        y_scale(s).start()
        for a in range(2):
            y_copy(s + a).start()

    def keep_half(s):
        h = (s // 2) % 2
        for step in range(2):
            @pl.when(s == 2 * step)
            def _():
                turn(1, step)

        product(1, h, acc.at[pl.ds(s, 2)])

    def settle(s, sources):
        h = (s // 2) % 2
        r, f = pick(unit_r, unit_of(s)), pick(unit_f, unit_of(s))
        y_copy(s).wait_recv()

        @pl.when(s % 2 == 0)
        def _():
            y_scale(s).wait_recv()

        for way in range(sources):
            for copy in w_copies(s, way):
                copy.wait_recv()
        top = jnp.zeros((1, acc.shape[2]), jnp.float32)
        for k in range(4):
            at = pl.ds(k * part, part)
            value = acc[s, at, :] + unscaled(y_in.at[s], y_in_s.at[s], at)
            for way in range(sources):
                value += unscaled(w_in.at[way, s], w_in_s.at[way, s], at)
            acc[s, at, :] = value
            if sources < 2:
                top = highest(top, value)
        if sources < 2:
            put(acc.at[s], top, w_out.at[s], w_out_s.at[s])
            for copy in w_copies(s, sources):
                copy.start()
            return

        @pl.when(r == 0)
        def _():
            for e in range(experts):
                result[place(f, h, e)] = acc[s, :, e * SUB : (e + 1) * SUB]
            for copy in stores(f, h):
                copy.start()

        @pl.when(r != 0)
        def _():
            for copy in f_copies(s, r, f, h):
                copy.start()

    turn(0, 0)
    for copy in segments:
        copy.wait()
    for a in range(2):
        loads[units[a][1]].wait()
        cover(*units[a], a)
    ready(0, 0)
    pl.semaphore_wait(barrier, 4 + len(others))
    for f in range(n_ff):
        g_copy(2, f).start()
        g_copy(1, f).start()

    lags = (JOIN, JOIN + MERGE, JOIN + LAST)

    @pl.loop(0, count + lags[2])
    def _(i):
        for sources, role in enumerate((feeder, merger, target)):
            @pl.when(role & (i >= lags[sources]) & (i < count + lags[sources]))
            def _():
                settle(i - lags[sources], sources)

        @pl.when((i < count) & (i % 2 == 0))
        def _():
            form(i)

        @pl.when((i < count) & (i % 2 == 1))
        def _():
            keep_half(i - 1)

    blocks = [(f, h) for f in range(n_ff) for h in range(2)]

    @pl.when(z != t)
    def _():
        for f, h in blocks:
            for e, copy in enumerate(f_copies(0, 1, f, h)):
                copy.wait_recv()
            for copy in stores(f, h):
                copy.start()

    @pl.loop(0, count)
    def _(s):
        r = pick(unit_r, unit_of(s))
        y_copy(s).wait_send()

        @pl.when(s % 2 == 0)
        def _():
            y_scale(s).wait_send()

        @pl.when(z != t)
        def _():
            for copy in w_copies(s, 0):
                copy.wait_send()

        @pl.when((z == t) & (r != 0))
        def _():
            for copy in f_copies(s, r, 0, 0):
                copy.wait_send()

    for f in range(n_ff):
        for r in range(1, 4):
            g_copy(r, f).wait_send()
    for f, h in blocks:
        for copy in stores(f, h):
            copy.wait()


def kernel_device(n_dp, n_t, tokens, cotangent, seg_start, seg_length):
    rows, width = tokens.shape
    ff = cotangent.shape[1]
    experts = seg_start.shape[1]
    half = width // 2
    tall = half // 2
    n_ff = ff // SUB
    count = 2 * n_t * n_ff
    wide = experts * SUB
    dma = pltpu.SemaphoreType.DMA
    anywhere = pl.BlockSpec(memory_space=pl.ANY)
    data = pltpu.VMEM((count, tall, wide), jnp.int16)
    scale = pltpu.VMEM((count, 1, wide), jnp.float32)
    out = pl.pallas_call(
        functools.partial(grad_kernel, n_dp, n_t, experts),
        out_shape=jax.ShapeDtypeStruct((experts, half, ff), jnp.float32),
        in_specs=[anywhere] * 4,
        out_specs=anywhere,
        scratch_shapes=[
            pltpu.VMEM((2, 2, rows, tall), tokens.dtype),
            pltpu.VMEM((2, 2, tall, rows), tokens.dtype),
            pltpu.VMEM((n_t, n_ff, rows, SUB), cotangent.dtype),
            pltpu.VMEM((rows, 2 * wide), cotangent.dtype),
            pltpu.VMEM((count, tall, wide), jnp.float32),
            pltpu.VMEM((2, tall, wide), jnp.float32),
            pltpu.VMEM((experts, half, ff), jnp.float32),
            data, data, data,
            pltpu.VMEM((2, count, tall, wide), jnp.int16),
            scale, scale, scale,
            pltpu.VMEM((2, count, 1, wide), jnp.float32),
            dma((n_ff + 4,)),
            dma((n_t, n_ff)),
            dma((n_t, n_ff)),
            dma((2, count)),
            dma((2, count)),
            dma((2, count)),
            dma((2, 2, count)),
            dma((count, experts)),
            dma((n_ff, 2, experts)),
            dma((n_ff, 2, experts)),
            pltpu.SMEM(seg_start.shape, jnp.int32),
            pltpu.SMEM(seg_length.shape, jnp.int32),
            dma((2,)),
        ],
        compiler_params=pltpu.CompilerParams(
            collective_id=0, has_side_effects=True, vmem_limit_bytes=67043328
        ),
    )(tokens, cotangent, seg_start, seg_length)
    return out.transpose(1, 0, 2)


def solution(mesh):
    n_dp, n_t = mesh.shape["dp"], mesh.shape["tensor"]
    body = plain_device
    if n_t == 4 and n_dp == 2 * n_t:
        body = functools.partial(kernel_device, n_dp, n_t)
    in_specs = (P("dp", "tensor"), P("dp", "tensor"), P("dp", None), P("dp", None))
    out_specs = P("dp", None, "tensor")
    return jax.shard_map(
        body, mesh=mesh, in_specs=in_specs, out_specs=out_specs, check_vma=False
    )
```
